32 devices in a mesh: rows: 8 (over y, x, core), model: 4 (over z).
Axes of the slice: x: 2, y: 2, z: 4, core: 2. Of those that a mesh axis runs over, the one named last changes fastest.
Arguments:
- one_query: float32 [5120, 5120], P('rows', 'model'), may hold values from -0.125 to 0.125
- other_query: float32 [5120, 5120], P('rows', 'model'), may hold values from -0.078125 to 0.078125
- one_key: float32 [5120, 5120], P('rows', 'model'), may hold values from -0.125 to 0.125
- other_key: float32 [5120, 5120], P('rows', 'model'), may hold values from -0.078125 to 0.078125
- one_value: float32 [5120, 5120], P('rows', 'model'), may hold values from -0.125 to 0.125
- other_value: float32 [5120, 5120], P('rows', 'model'), may hold values from -0.078125 to 0.078125
- mix_share: float32 [5120], P('rows'), may hold values from 0.2 to 0.8
- norm_gain: float32 [5120], P('rows'), may hold values from 0.25 to 1.75
Outputs:
- final_query: bfloat16 [5120, 5120], P(None, 'model')
- final_key: bfloat16 [5120, 5120], P(None, 'model')
- final_value: bfloat16 [5120, 5120], P(None, 'model')
- factor_query: float32 [5120], P('model')
- factor_key: float32 [5120], P('model')
- factor_value: float32 [5120], P('model')
The draws below stay inside these ranges and needn't reach their ends.
All inputs are finite; a program needn't handle non-finite values. Where the reference program divides by a largest or mean magnitude, that divisor is 1e-20 or more.
Results may differ from the reference program's by a relative error of at most 0.001.
Values may be sent and summed in bfloat16 or wider, within the bound.
No kernel may reach another device: no remote copies, remote signals or barrier semaphores. Data moves between devices by JAX's collectives and lax.ppermute only.
A program may use at most 192 MiB of HBM per device.

```python
import jax
import jax.numpy as jnp

D_MODEL = 5120
Q_DIM = 5120
KV_DIM = 5120


def raised(array, stream_key, source, target, blocks, factor):
    def block_of(position):
        return (jnp.arange(array.shape[position]) // (array.shape[position] // blocks)).reshape((-1,) + (1,) * (array.ndim - 1 - position))

    near = jax.random.permutation(stream_key, blocks)[block_of(target)]
    far = (block_of(target) + blocks // 2) % blocks
    return jnp.where((block_of(source) == near) | (block_of(source) == far), factor * array, array)


def level_of(rng, dims, pieces, least, high):
    gain = 1.0
    for position, blocks in pieces:
        draws = jax.random.uniform(jax.random.fold_in(jax.random.fold_in(rng, 6), position), (blocks,), jnp.float32, least / len(pieces), high / len(pieces))
        gain = gain * jnp.repeat(jnp.exp(draws), dims[position] // blocks).reshape((-1,) + (1,) * (len(dims) - 1 - position))
    return gain


def normal_values(rng, dims, spread, bound, split=(), kind=jnp.bfloat16):
    level = level_of(rng, dims, split, -0.22, 0.18) if split else 1.0
    result = jax.random.normal(rng, dims, jnp.float32) * spread * level
    return jnp.minimum(jnp.maximum(result, -bound), bound).astype(kind)


def noise_with(rng, dims, deviation, most, split, heavy, kind=jnp.bfloat16):
    entries = deviation * jax.random.normal(rng, dims, jnp.float32)
    if split:
        entries = entries * level_of(rng, dims, split, -0.22, 0.18)
    return jnp.clip(raised(entries, jax.random.fold_in(rng, 3), *heavy), -most, most).astype(kind)


def setup_inputs(seed: int = 0) -> dict:
    arg_keys = jax.random.split(jax.random.key(seed), 9)
    return {
        "one_query": noise_with(arg_keys[0], (D_MODEL, Q_DIM), D_MODEL ** -0.5, 0.125, ((0, 8), (1, 4)), (0, 1, 8, 2.0), jnp.float32),
        "other_query": normal_values(arg_keys[1], (D_MODEL, Q_DIM), D_MODEL ** -0.5, 0.078125, ((0, 8), (1, 4)), jnp.float32),
        "one_key": noise_with(arg_keys[2], (D_MODEL, KV_DIM), D_MODEL ** -0.5, 0.125, ((0, 8), (1, 4)), (0, 1, 8, 2.0), jnp.float32),
        "other_key": normal_values(arg_keys[3], (D_MODEL, KV_DIM), D_MODEL ** -0.5, 0.078125, ((0, 8), (1, 4)), jnp.float32),
        "one_value": noise_with(arg_keys[4], (D_MODEL, KV_DIM), D_MODEL ** -0.5, 0.125, ((0, 8), (1, 4)), (0, 1, 8, 2.0), jnp.float32),
        "other_value": normal_values(arg_keys[5], (D_MODEL, KV_DIM), D_MODEL ** -0.5, 0.078125, ((0, 8), (1, 4)), jnp.float32),
        "mix_share": jnp.clip(0.2 + 0.6 * jax.random.uniform(arg_keys[6], (D_MODEL,), jnp.float32) ** level_of(arg_keys[6], (D_MODEL,), ((0, 8),), -0.2, 0.2), 0.2, 0.8),
        "norm_gain": jnp.clip(1.0 + 0.15 * jax.random.normal(arg_keys[7], (D_MODEL,), jnp.float32), 0.25, 1.75),
    }


def reference(one_query, other_query, one_key, other_key, one_value, other_value, mix_share, norm_gain):
    result_query = mix_share[:, None] * one_query + (1.0 - mix_share[:, None]) * other_query
    result_key = mix_share[:, None] * one_key + (1.0 - mix_share[:, None]) * other_key
    result_value = mix_share[:, None] * one_value + (1.0 - mix_share[:, None]) * other_value
    result_gained_query = result_query * norm_gain[:, None]
    result_gained_key = result_key * norm_gain[:, None]
    result_gained_value = result_value * norm_gain[:, None]
    factor_query = jnp.max(jnp.abs(result_gained_query), axis=0)
    final_query = (result_gained_query / factor_query).astype(jnp.bfloat16)
    factor_key = jnp.max(jnp.abs(result_gained_key), axis=0)
    final_key = (result_gained_key / factor_key).astype(jnp.bfloat16)
    factor_value = jnp.max(jnp.abs(result_gained_value), axis=0)
    final_value = (result_gained_value / factor_value).astype(jnp.bfloat16)
    return final_query, final_key, final_value, factor_query, factor_key, factor_value
```

```python
import functools

import jax
import jax.numpy as jnp
from jax import lax
from jax.experimental import pallas as pl
from jax.experimental.pallas import tpu as pltpu
from jax.sharding import PartitionSpec as P


def place_body(count, rows, *refs):
    starts, pieces = refs[0], refs[1 : 1 + count]
    out, *slots, into, back = refs[-(count + 3) :]
    ins = [pltpu.make_async_copy(pieces[k], slots[k], into.at[k]) for k in range(count)]
    outs = []
    for k in range(count):
        at = pl.multiple_of(starts[k] * 16, 16)
        outs.append(pltpu.make_async_copy(slots[k], out.at[pl.ds(at, rows[k])], back.at[k]))
        ins[k].start()
    for k in range(count):
        ins[k].wait()
        outs[k].start()
    for k in range(count):
        outs[k].wait()


def place(pieces, starts, shape, filled=None):
    count = len(pieces)
    anywhere = pl.BlockSpec(memory_space=pltpu.HBM)
    operands = [jnp.stack(starts).astype(jnp.int32) // 16, *pieces]
    aliases = {}
    if filled is not None:
        aliases = {len(operands): 0}
        operands.append(filled)
    moved = 2 * 2 * sum(p.size for p in pieces)
    return pl.pallas_call(
        functools.partial(place_body, count, [p.shape[0] for p in pieces]),
        out_shape=jax.ShapeDtypeStruct(shape, jnp.bfloat16),
        in_specs=[pl.BlockSpec(memory_space=pltpu.SMEM)] + [anywhere] * (len(operands) - 1),
        out_specs=anywhere,
        scratch_shapes=[pltpu.VMEM(p.shape, jnp.bfloat16) for p in pieces]
        + [pltpu.SemaphoreType.DMA((count,)), pltpu.SemaphoreType.DMA((count,))],
        input_output_aliases=aliases,
        cost_estimate=pl.CostEstimate(flops=0, bytes_accessed=moved, transcendentals=0),
    )(*operands)


def grid_of(n):
    pair = 2 if n % 2 == 0 else 1
    rest = n // pair
    inner = 2 if rest % 2 == 0 else 1
    return rest // inner, inner, pair


def shift(x, n, axis, by):
    dims = grid_of(n)
    table = []
    for i in range(n):
        o, rest = divmod(i, dims[1] * dims[2])
        at = [o, *divmod(rest, dims[2])]
        at[axis] = (at[axis] + by) % dims[axis]
        table.append((i, (at[0] * dims[1] + at[1]) * dims[2] + at[2]))
    return lax.ppermute(x, "rows", table)


def gather_all(halves, n, me):
    outer, inner, pair = grid_of(n)
    size = halves[0].shape[0]
    mine = (me // (inner * pair), (me // pair) % inner, me % pair)
    dims = (outer, inner, pair)

    def row(offsets, half):
        at = [(mine[a] - offsets[a]) % dims[a] for a in range(3)]
        return ((at[0] * inner + at[1]) * pair + at[2]) * (2 * size) + half * size

    early, late = [], []
    for half in (0, 1):
        early.append((halves[half], (0, 0, 0), half))
    got = {}
    for by in range(1, inner):
        for half in (0, 1):
            got[(0, by, half)] = shift(halves[half], n, 1, by)
    for by in range(1, outer):
        for half in (1, 0):
            got[(by, 0, half)] = shift(halves[half], n, 0, by)
    for (o, i, half), piece in got.items():
        early.append((piece, (o, i, 0), half))
    for o in range(1, outer):
        for i in range(1, inner):
            late.append((shift(got[(0, i, 0)], n, 0, o), (o, i, 0), 0))
            late.append((shift(got[(o, 0, 1)], n, 1, i), (o, i, 0), 1))

    def both(pieces):
        every = list(pieces)
        for by in range(1, pair):
            for piece, (o, i, _), half in pieces:
                every.append((shift(piece, n, 2, by), (o, i, by), half))
        return [p for p, _, _ in every], [row(at, half) for _, at, half in every]

    return both(early), both(late)


def gains(one, other, mix_share, norm_gain):
    return (mix_share[:, None] * one + (1.0 - mix_share[:, None]) * other) * norm_gain[:, None]


def factors_of(gained):
    tops = jnp.stack([jnp.max(jnp.abs(g), axis=0) for g in gained])
    return jnp.max(lax.all_gather(tops, "rows", axis=0), axis=0)


def halves_of(gained, factor):
    half = gained.shape[0] // 2
    return [(gained[h * half : (h + 1) * half] / factor).astype(jnp.bfloat16) for h in (0, 1)]


def local(n, *args):
    ones, others, mix_share, norm_gain = list(args[0:6:2]), list(args[1:6:2]), args[6], args[7]
    me = lax.axis_index("rows")
    first = gains(ones[0], others[0], mix_share, norm_gain)
    factors = [factors_of([first])[0]]
    halves = [halves_of(first, factors[0])]
    (ones[1:], others[1:], halves[0]) = lax.optimization_barrier((ones[1:], others[1:], halves[0]))
    rest = [gains(ones[k], others[k], mix_share, norm_gain) for k in (1, 2)]
    tops = factors_of(rest)
    factors += [tops[0], tops[1]]
    halves += [halves_of(rest[k - 1], factors[k]) for k in (1, 2)]
    plans = [gather_all(halves[k], n, me) for k in range(3)]
    finals = []
    for early, late in plans:
        shape = (first.shape[0] * n, first.shape[1])
        out = place(*early, shape)
        if late[0]:
            out = place(*late, shape, out)
        finals.append(out)
    return (*finals, *factors)


def solution(mesh):
    whole = P("rows", "model")
    return jax.shard_map(
        functools.partial(local, mesh.shape["rows"]),
        mesh=mesh,
        in_specs=(whole,) * 6 + (P("rows"),) * 2,
        out_specs=(P(None, "model"),) * 3 + (P("model"),) * 3,
        check_vma=False,
    )
```

```python
import functools

import jax
import jax.numpy as jnp
from jax import lax
from jax.experimental import pallas as pl
from jax.experimental.pallas import tpu as pltpu
from jax.sharding import PartitionSpec as P


def place_body(count, rows, *refs):
    starts, pieces = refs[0], refs[1 : 1 + count]
    out, *slots, into, back = refs[-(count + 3) :]
    ins = [pltpu.make_async_copy(pieces[k], slots[k], into.at[k]) for k in range(count)]
    outs = []
    for k in range(count):
        at = pl.multiple_of(starts[k] * 16, 16)
        outs.append(pltpu.make_async_copy(slots[k], out.at[pl.ds(at, rows[k])], back.at[k]))
        ins[k].start()
    for k in range(count):
        ins[k].wait()
        outs[k].start()
    for k in range(count):
        outs[k].wait()


def place(pieces, starts, shape, filled=None):
    count = len(pieces)
    anywhere = pl.BlockSpec(memory_space=pltpu.HBM)
    operands = [jnp.stack(starts).astype(jnp.int32) // 16, *pieces]
    aliases = {}
    if filled is not None:
        aliases = {len(operands): 0}
        operands.append(filled)
    moved = 2 * 2 * sum(p.size for p in pieces)
    return pl.pallas_call(
        functools.partial(place_body, count, [p.shape[0] for p in pieces]),
        out_shape=jax.ShapeDtypeStruct(shape, jnp.bfloat16),
        in_specs=[pl.BlockSpec(memory_space=pltpu.SMEM)] + [anywhere] * (len(operands) - 1),
        out_specs=anywhere,
        scratch_shapes=[pltpu.VMEM(p.shape, jnp.bfloat16) for p in pieces]
        + [pltpu.SemaphoreType.DMA((count,)), pltpu.SemaphoreType.DMA((count,))],
        input_output_aliases=aliases,
        cost_estimate=pl.CostEstimate(flops=0, bytes_accessed=moved, transcendentals=0),
    )(*operands)


def grid_of(n):
    pair = 2 if n % 2 == 0 else 1
    rest = n // pair
    inner = 2 if rest % 2 == 0 else 1
    return rest // inner, inner, pair


def shift(x, n, axis, by):
    dims = grid_of(n)
    table = []
    for i in range(n):
        o, rest = divmod(i, dims[1] * dims[2])
        at = [o, *divmod(rest, dims[2])]
        at[axis] = (at[axis] + by) % dims[axis]
        table.append((i, (at[0] * dims[1] + at[1]) * dims[2] + at[2]))
    return lax.ppermute(x, "rows", table)


def gather_all(halves, n, me):
    outer, inner, pair = grid_of(n)
    size = halves[0].shape[0]
    mine = (me // (inner * pair), (me // pair) % inner, me % pair)
    dims = (outer, inner, pair)

    def row(offsets, half):
        at = [(mine[a] - offsets[a]) % dims[a] for a in range(3)]
        return ((at[0] * inner + at[1]) * pair + at[2]) * (2 * size) + half * size

    early, late = [], []
    for half in (0, 1):
        early.append((halves[half], (0, 0, 0), half))
    got = {}
    for by in range(1, inner):
        for half in (0, 1):
            got[(0, by, half)] = shift(halves[half], n, 1, by)
    for by in range(1, outer):
        for half in (1, 0):
            got[(by, 0, half)] = shift(halves[half], n, 0, by)
    for (o, i, half), piece in got.items():
        early.append((piece, (o, i, 0), half))
    for o in range(1, outer):
        for i in range(1, inner):
            late.append((shift(got[(0, i, 0)], n, 0, o), (o, i, 0), 0))
            late.append((shift(got[(o, 0, 1)], n, 1, i), (o, i, 0), 1))

    def both(pieces):
        every = list(pieces)
        for by in range(1, pair):
            for piece, (o, i, _), half in pieces:
                every.append((shift(piece, n, 2, by), (o, i, by), half))
        return [p for p, _, _ in every], [row(at, half) for _, at, half in every]

    return both(early), both(late)


def gains(one, other, mix_share, norm_gain):
    return (mix_share[:, None] * one + (1.0 - mix_share[:, None]) * other) * norm_gain[:, None]


def factors_of(gained):
    tops = jnp.stack([jnp.max(jnp.abs(g), axis=0) for g in gained])
    return jnp.max(lax.all_gather(tops, "rows", axis=0), axis=0)


def halves_of(gained, factor):
    half = gained.shape[0] // 2
    return [(gained[h * half : (h + 1) * half] / factor).astype(jnp.bfloat16) for h in (0, 1)]


def local(n, *args):
    ones, others, mix_share, norm_gain = list(args[0:6:2]), list(args[1:6:2]), args[6], args[7]
    me = lax.axis_index("rows")
    gained = [gains(one, other, mix_share, norm_gain) for one, other in zip(ones, others)]
    tops = factors_of(gained)
    factors = [tops[k] for k in range(3)]
    halves = [halves_of(gained[k], factors[k]) for k in range(3)]
    plans = [gather_all(halves[k], n, me) for k in range(3)]
    finals = []
    for early, late in plans:
        shape = (ones[0].shape[0] * n, ones[0].shape[1])
        out = place(*early, shape)
        if late[0]:
            out = place(*late, shape, out)
        finals.append(out)
    return (*finals, *factors)


def solution(mesh):
    whole = P("rows", "model")
    return jax.shard_map(
        functools.partial(local, mesh.shape["rows"]),
        mesh=mesh,
        in_specs=(whole,) * 6 + (P("rows"),) * 2,
        out_specs=(P(None, "model"),) * 3 + (P("model"),) * 3,
        check_vma=False,
    )
```
